32 devices in a mesh: b: 1 (over z), rep: 4 (over y), col: 4 (over x), row: 2 (over core).
Axes of the slice: x: 4, y: 4, z: 1, core: 2. Of those that a mesh axis runs over, the one named last changes fastest.
The devices are a block of a 4x4x8 slice.
Arguments:
- a_blocks: float32 [36, 36, 128, 128], P(('b', 'row'), 'col')
Outputs:
- output: float32 [36, 36, 128, 128], P(('b', 'row'), 'col')
All inputs are finite; a program needn't handle non-finite values.
Results may differ from the reference program's by a relative error of at most 0.001.
Values sent between devices are 32-bit elements.
A program may use at most 768 MiB of HBM per device.

```python
import jax
import jax.numpy as jnp
from jax import lax

N = 4608
NB = 128
ROW = 2
COL = 4
RANK = N // 8
NUM_BLK = N // NB
ROW_BLK = NUM_BLK // ROW
COL_BLK = NUM_BLK // COL


def to_cyclic(natural):
    grid_view = natural.reshape(ROW_BLK, ROW, NB, COL_BLK, COL, NB)
    return grid_view.transpose(1, 0, 4, 3, 2, 5).reshape(NUM_BLK, NUM_BLK, NB, NB)


def from_cyclic(blocks):
    grid_view = blocks.reshape(ROW, ROW_BLK, COL, COL_BLK, NB, NB)
    return grid_view.transpose(1, 0, 4, 3, 2, 5).reshape(N, N)


def setup_inputs(seed: int = 0, part: int = 0) -> dict:
    base_key = jax.random.fold_in(jax.random.key(seed), part)
    factor = jax.random.normal(base_key, (N, RANK), jnp.float32)
    gram_mat = jnp.dot(factor, factor.T, precision=lax.Precision.HIGHEST, preferred_element_type=jnp.float32)
    spd_mat = 0.5 * (gram_mat + gram_mat.T) + RANK * jnp.eye(N, dtype=jnp.float32)
    return {"a_blocks": to_cyclic(spd_mat)}


def reference(a_blocks):
    lower_fac = jnp.tril(jnp.linalg.cholesky(from_cyclic(a_blocks)))
    return to_cyclic(lower_fac)
```

```python
import functools

import jax
import jax.numpy as jnp
from jax import lax
from jax.experimental import pallas as pl
from jax.experimental.pallas import tpu as pltpu
from jax.sharding import PartitionSpec as P

SUB = 8
MESH = pl.DeviceIdType.MESH


def dot_nt(lhs, rhs):
    return lax.dot_general(
        lhs, rhs, (((1,), (1,)), ((), ())),
        precision=lax.Precision.HIGHEST, preferred_element_type=jnp.float32,
    )


def lane_bcast(vec, lane):
    return jnp.broadcast_to(vec[:, lane:lane + 1], vec.shape)


def sub_bcast(vec, row):
    return jnp.broadcast_to(vec[row:row + 1, :], vec.shape)


def tree_sum(terms):
    while len(terms) > 1:
        terms = [sum(terms[a:a + 2][1:], terms[a]) for a in range(0, len(terms), 2)]
    return terms[0]


def factor_block(mat, put_u, put_w):
    panels = len(mat)
    shape = mat[0].shape
    lane = lax.broadcasted_iota(jnp.int32, shape, 1)
    sub = lax.broadcasted_iota(jnp.int32, shape, 0)
    aug = [jnp.where(lane == sub + SUB * q, 1.0, 0.0).astype(jnp.float32) for q in range(panels)]
    for p in range(panels):
        base = SUB * p
        cols = [lane_bcast(mat[p], base + j) for j in range(SUB)]
        piv = {(i, j): sub_bcast(cols[j], i) for j in range(SUB) for i in range(j, SUB)}
        rows_m = [sub_bcast(mat[p], i) for i in range(SUB)]
        rows_x = [sub_bcast(aug[p], i) for i in range(SUB)]
        low, inv, root = {}, [], []
        for j in range(SUB):
            inv.append(1.0 / piv[j, j])
            root.append(lax.rsqrt(piv[j, j]))
            for i in range(j + 1, SUB):
                low[i, j] = piv[i, j] * inv[j]
            for i in range(j + 1, SUB):
                for k in range(j + 1, i + 1):
                    piv[i, k] = piv[i, k] - low[i, j] * piv[k, j]
                rows_m[i] = rows_m[i] - low[i, j] * rows_m[j]
                rows_x[i] = rows_x[i] - low[i, j] * rows_x[j]
        u_rows = rows_m[0] * root[0]
        w_rows = rows_x[0] * root[0]
        for i in range(1, SUB):
            u_rows = jnp.where(sub == i, rows_m[i] * root[i], u_rows)
            w_rows = jnp.where(sub == i, rows_x[i] * root[i], w_rows)
        put_u(p, u_rows)
        put_w(p, w_rows)
        if p + 1 == panels:
            break
        back_m = [rows_m[i] * inv[i] for i in range(SUB)]
        back_x = [rows_x[i] * inv[i] for i in range(SUB)]
        for i in range(SUB - 2, -1, -1):
            for j in range(SUB - 1, i, -1):
                back_m[i] = back_m[i] - low[j, i] * back_m[j]
                back_x[i] = back_x[i] - low[j, i] * back_x[j]
        for q in range(p + 1, panels):
            coef = [lane_bcast(mat[q], base + j) for j in range(SUB)]
            mat[q] = mat[q] - tree_sum([coef[j] * back_m[j] for j in range(SUB)])
            aug[q] = aug[q] - tree_sum([coef[j] * back_x[j] for j in range(SUB)])


def kernel(sizes, a_ref, out_ref, l_st, w_st, a_row, u_st, d_buf, u_buf, zero_buf,
           l_sem, w_sem, a_sem, out_sem, send_sem):
    row_size, col_size, rep_size = sizes
    rows_blk, cols_blk, blk, _ = a_ref.shape
    num = rows_blk * row_size
    chips = col_size * rep_size
    ring = chips * row_size
    slots = a_row.shape[0]
    twin = max(num - ring, 0)
    row, col, rep = lax.axis_index("row"), lax.axis_index("col"), lax.axis_index("rep")

    def snake(y, x):
        return jnp.where(y % 2 == 0, x, col_size - 1 - x)

    me = (rep * col_size + snake(rep, col)) * row_size + row

    def place(dev):
        chip = dev // row_size
        y = chip // col_size
        return {"rep": y, "col": snake(y, chip % col_size), "row": dev % row_size}

    def last_row(dev):
        return jnp.where(dev < twin, dev + ring, dev)

    def packed(big, small):
        return small * num - (small * (small - 1)) // 2 + big - small

    def send(src, dst, sem, where):
        pltpu.make_async_remote_copy(
            src_ref=src, dst_ref=dst, send_sem=send_sem, recv_sem=sem,
            device_id=where, device_id_type=MESH,
        ).start()

    def wait_block(ref, sem):
        pltpu.make_async_copy(ref, ref, sem).wait()

    barrier = pltpu.get_barrier_semaphore()

    @pl.loop(1, ring)
    def _(t):
        pl.semaphore_signal(barrier, inc=1, device_id=place((me + t) % ring), device_id_type=MESH)

    zero_buf[...] = jnp.zeros_like(zero_buf)
    u_st[...] = jnp.zeros_like(u_st)

    @pl.loop(0, rows_blk)
    def _(i):
        @pl.loop(0, cols_blk)
        def _(j):
            @pl.when(j * col_size + col > i * row_size + row)
            def _():
                pltpu.make_async_copy(zero_buf, out_ref.at[i, j], out_sem).start()

    pl.semaphore_wait(barrier, ring - 1)

    @pl.loop(0, cols_blk)
    def _(jj):
        for to_col in range(col_size):
            for s in range(slots):
                dest = (rep * col_size + snake(rep, to_col)) * row_size + row
                big = dest + s * ring
                j = jj * col_size + col

                @pl.when((big < num) & (j <= big))
                def _():
                    src, dst = a_ref.at[big // row_size, jj], a_row.at[s, j]

                    @pl.when(col == to_col)
                    def _():
                        pltpu.make_async_copy(src, dst, a_sem.at[s, j]).start()

                    @pl.when(col != to_col)
                    def _():
                        send(src, dst, a_sem.at[s, j], {"col": to_col})

    def to_later(src, dst, sem, big, lo, hi):
        @pl.loop(lo, hi)
        def _(t):
            dest = (me + t) % ring

            @pl.when(last_row(dest) > big)
            def _():
                send(src, dst, sem, place(dest))

    def to_output(idx, big, small):
        src, dst = l_st.at[idx], out_ref.at[big // row_size, small // col_size]
        to_col = small % col_size
        for to_rep in range(rep_size):
            here = (rep == to_rep) & (col == to_col)

            @pl.when(here)
            def _():
                pltpu.make_async_copy(src, dst, out_sem).start()

            @pl.when(jnp.logical_not(here))
            def _():
                send(src, dst, out_sem, {"rep": to_rep, "col": to_col})

    @pl.loop(-1, num - 1)
    def _(i):
        @pl.when((i >= 0) & (last_row(me) > i) & (i % ring != me))
        def _():
            wait_block(w_st.at[i], w_sem.at[i])

        @pl.loop(0, slots)
        def _(s):
            big = me + s * ring
            idx = packed(big, i)
            critical = big == i + 1
            follow = (big < num) & (big > i) & (i >= 0)

            @pl.when(follow)
            def _():
                wait_block(a_row.at[s, i], a_sem.at[s, i])
                gap = big - i
                half = pl.multiple_of((1 - gap % 2) * blk, blk)
                l_st[idx] = dot_nt(a_row[s, i] - u_st[s, gap // 2, :, pl.ds(half, blk)], w_st[i])
                to_later(l_st.at[idx], l_st.at[idx], l_sem.at[idx], big, 1, jnp.where(critical, 2, ring))

                @pl.when(jnp.logical_not(critical))
                def _():
                    to_output(idx, big, i)

                @pl.loop(jnp.maximum(i, jnp.where(s > 0, me, -1)) + 1, big)
                def _(j):
                    there = packed(j, i)
                    wait_block(l_st.at[there], l_sem.at[there])

                mine = l_st[idx]

                @pl.loop(0, (gap + 1) // 2)
                def _(g):
                    pair = l_st[pl.ds(idx - 2 * g - 1, 2)].reshape(2 * blk, blk)
                    u_st[s, g] = u_st[s, g] + dot_nt(mine, pair)

            @pl.when(critical & (big < num))
            def _():
                wait_block(a_row.at[s, big], a_sem.at[s, big])
                d_buf[...] = a_row[s, big] - u_st[s, 0, :, blk:2 * blk]

                def put_u(p, val):
                    u_buf[SUB * p:SUB * p + SUB, :] = val

                def put_w(p, val):
                    w_st[big, SUB * p:SUB * p + SUB, :] = val

                factor_block([d_buf[SUB * q:SUB * q + SUB, :] for q in range(blk // SUB)], put_u, put_w)
                to_later(w_st.at[big], w_st.at[big], w_sem.at[big], big, 1, ring)

                @pl.when(follow)
                def _():
                    to_later(l_st.at[idx], l_st.at[idx], l_sem.at[idx], big, 2, ring)
                    to_output(idx, big, i)

                lane = lax.broadcasted_iota(jnp.int32, (blk, blk), 1)
                sub = lax.broadcasted_iota(jnp.int32, (blk, blk), 0)
                diag = packed(big, big)
                l_st[diag] = jnp.where(lane <= sub, u_buf[...].T, 0.0)
                to_output(diag, big, big)

    total = 0
    for s in range(slots):
        big = me + s * ring
        targets = num - jnp.maximum(big + 1, twin) - jnp.where(last_row(me) > big, 1, 0)
        own = (big - col + col_size) // col_size
        sent = (big + 1) * targets + (big + 1) * rep_size - own
        total = total + jnp.where(big < num, sent, 0)
        for to_col in range(col_size):
            other = (rep * col_size + snake(rep, to_col)) * row_size + row + s * ring
            dealt = (other - col + col_size) // col_size
            total = total + jnp.where((other < num) & (to_col != col), dealt, 0)
    chunk = 16

    @pl.loop(0, total // chunk)
    def _(t):
        wait_block(l_st.at[0:chunk], send_sem)

    @pl.loop(0, total % chunk)
    def _(t):
        wait_block(l_st.at[0], send_sem)

    wait_block(out_ref, out_sem)


def solution(mesh):
    sizes = tuple(mesh.shape[axis] for axis in ("row", "col", "rep"))
    grid_spec = P(("b", "row"), "col")

    def local_factor(a_loc):
        rows_blk, cols_blk, blk, _ = a_loc.shape
        num = rows_blk * sizes[0]
        ring = sizes[0] * sizes[1] * sizes[2]
        slots = -(-num // ring)
        assert slots <= 2
        f32 = jnp.float32
        dma = pltpu.SemaphoreType.DMA
        tri = num * (num + 1) // 2
        return pl.pallas_call(
            functools.partial(kernel, sizes),
            out_shape=jax.ShapeDtypeStruct(a_loc.shape, f32),
            in_specs=[pl.BlockSpec(memory_space=pl.ANY)],
            out_specs=pl.BlockSpec(memory_space=pl.ANY),
            scratch_shapes=[
                pltpu.VMEM((tri, blk, blk), f32),
                pltpu.VMEM((num, blk, blk), f32),
                pltpu.VMEM((slots, num, blk, blk), f32),
                pltpu.VMEM((slots, (num + 1) // 2, blk, 2 * blk), f32),
                pltpu.VMEM((blk, blk), f32),
                pltpu.VMEM((blk, blk), f32),
                pltpu.VMEM((blk, blk), f32),
                dma((tri,)),
                dma((num,)),
                dma((slots, num)),
                dma,
                dma,
            ],
            compiler_params=pltpu.CompilerParams(
                collective_id=0, has_side_effects=True, vmem_limit_bytes=67043328,
            ),
        )(a_loc)

    return jax.shard_map(local_factor, mesh=mesh, in_specs=grid_spec, out_specs=grid_spec, check_vma=False)
```

```python
import functools

import jax
import jax.numpy as jnp
from jax import lax
from jax.experimental import pallas as pl
from jax.experimental.pallas import tpu as pltpu
from jax.sharding import PartitionSpec as P

SUB = 8
NEAR = 2
UNROLL = 4
MESH = pl.DeviceIdType.MESH


def dot_nt(lhs, rhs):
    return lax.dot_general(
        lhs, rhs, (((1,), (1,)), ((), ())),
        precision=lax.Precision.HIGHEST, preferred_element_type=jnp.float32,
    )


def lane_bcast(vec, lane):
    return jnp.broadcast_to(vec[:, lane:lane + 1], vec.shape)


def sub_bcast(vec, row):
    return jnp.broadcast_to(vec[row:row + 1, :], vec.shape)


def tree_sum(terms):
    while len(terms) > 1:
        terms = [sum(terms[a:a + 2][1:], terms[a]) for a in range(0, len(terms), 2)]
    return terms[0]


def factor_block(mat, put_u, put_w):
    panels = len(mat)
    shape = mat[0].shape
    lane = lax.broadcasted_iota(jnp.int32, shape, 1)
    sub = lax.broadcasted_iota(jnp.int32, shape, 0)
    aug = [jnp.where(lane == sub + SUB * q, 1.0, 0.0).astype(jnp.float32) for q in range(panels)]
    for p in range(panels):
        base = SUB * p
        cols = [lane_bcast(mat[p], base + j) for j in range(SUB)]
        piv = {(i, j): sub_bcast(cols[j], i) for j in range(SUB) for i in range(j, SUB)}
        rows_m = [sub_bcast(mat[p], i) for i in range(SUB)]
        rows_x = [sub_bcast(aug[p], i) for i in range(SUB)]
        low, inv, root = {}, [], []
        for j in range(SUB):
            inv.append(1.0 / piv[j, j])
            root.append(lax.rsqrt(piv[j, j]))
            for i in range(j + 1, SUB):
                low[i, j] = piv[i, j] * inv[j]
            for i in range(j + 1, SUB):
                for k in range(j + 1, i + 1):
                    piv[i, k] = piv[i, k] - low[i, j] * piv[k, j]
                rows_m[i] = rows_m[i] - low[i, j] * rows_m[j]
                rows_x[i] = rows_x[i] - low[i, j] * rows_x[j]
        u_rows = rows_m[0] * root[0]
        w_rows = rows_x[0] * root[0]
        for i in range(1, SUB):
            u_rows = jnp.where(sub == i, rows_m[i] * root[i], u_rows)
            w_rows = jnp.where(sub == i, rows_x[i] * root[i], w_rows)
        put_u(p, u_rows)
        put_w(p, w_rows)
        if p + 1 == panels:
            break
        back_m = [rows_m[i] * inv[i] for i in range(SUB)]
        back_x = [rows_x[i] * inv[i] for i in range(SUB)]
        for i in range(SUB - 2, -1, -1):
            for j in range(SUB - 1, i, -1):
                back_m[i] = back_m[i] - low[j, i] * back_m[j]
                back_x[i] = back_x[i] - low[j, i] * back_x[j]
        for q in range(p + 1, panels):
            coef = [lane_bcast(mat[q], base + j) for j in range(SUB)]
            mat[q] = mat[q] - tree_sum([coef[j] * back_m[j] for j in range(SUB)])
            aug[q] = aug[q] - tree_sum([coef[j] * back_x[j] for j in range(SUB)])


def kernel(sizes, a_ref, out_ref, l_st, w_st, a_row, d_acc, acc, u_buf, zero_buf, count,
           l_sem, w_sem, a_sem, out_sem, send_sem):
    row_size, col_size, rep_size = sizes
    rows_blk, cols_blk, blk, _ = a_ref.shape
    num = rows_blk * row_size
    chips = col_size * rep_size
    ring = chips * row_size
    slots = a_row.shape[0]
    twin = max(num - ring, 0)
    row, col, rep = lax.axis_index("row"), lax.axis_index("col"), lax.axis_index("rep")

    def snake(y, x):
        return jnp.where(y % 2 == 0, x, col_size - 1 - x)

    chip = rep * col_size + snake(rep, col)
    me = chip * row_size + row

    def place(other_chip, other_row):
        y = other_chip // col_size
        return {"rep": y, "col": snake(y, other_chip % col_size), "row": other_row}

    def last_row(dev):
        return jnp.where(dev < twin, dev + ring, dev)

    my_last = last_row(me)

    def packed(big, small):
        return (big * (big + 1)) // 2 + small

    def send(src, dst, sem, where):
        count[0] = count[0] + 1
        pltpu.make_async_remote_copy(
            src_ref=src, dst_ref=dst, send_sem=send_sem, recv_sem=sem,
            device_id=where, device_id_type=MESH,
        ).start()

    def wait_block(ref, sem):
        pltpu.make_async_copy(ref, ref, sem).wait()

    barrier = pltpu.get_barrier_semaphore()

    @pl.loop(1, ring)
    def _(t):
        dev = (me + t) % ring
        pl.semaphore_signal(
            barrier, inc=1, device_id=place(dev // row_size, dev % row_size), device_id_type=MESH)

    count[0] = 0
    zero_buf[...] = jnp.zeros_like(zero_buf)
    d_acc[...] = jnp.zeros_like(d_acc)

    @pl.loop(0, rows_blk)
    def _(i):
        @pl.loop(0, cols_blk)
        def _(j):
            @pl.when(j * col_size + col > i * row_size + row)
            def _():
                pltpu.make_async_copy(zero_buf, out_ref.at[i, j], out_sem).start()

    pl.semaphore_wait(barrier, ring - 1)

    def deal(jj):
        j = jj * col_size + col
        for to_col in range(col_size):
            for s in range(slots):
                big = (rep * col_size + snake(rep, to_col)) * row_size + row + s * ring

                @pl.when((big < num) & (j <= big))
                def _():
                    src, dst = a_ref.at[big // row_size, jj], a_row.at[s, j]

                    @pl.when(col == to_col)
                    def _():
                        pltpu.make_async_copy(src, dst, a_sem.at[s, j]).start()

                    @pl.when(col != to_col)
                    def _():
                        send(src, dst, a_sem.at[s, j], {"col": to_col})

    def to_partner(ref, sem, big):
        for other in range(row_size):
            @pl.when((row != other) & (last_row(chip * row_size + other) > big))
            def _():
                send(ref, ref, sem, {"row": other})

    def to_chips(ref, sem, big, lo, hi, both):
        @pl.loop(lo, hi)
        def _(t):
            dest = (chip + t) % chips
            for shift in range(row_size):
                core = (row + row_size - 1 - shift) % row_size
                wanted = last_row(dest * row_size + core) > big
                if shift < row_size - 1:
                    wanted = wanted & (t <= both)

                @pl.when(wanted)
                def _():
                    send(ref, ref, sem, place(dest, core))

    def own_output(idx, big, small, everyone):
        src, dst = l_st.at[idx], out_ref.at[big // row_size, small // col_size]
        to_col = small % col_size
        for to_rep in range(rep_size):
            dest = (to_rep * col_size + snake(jnp.int32(to_rep), to_col)) * row_size + row
            here = dest == me

            @pl.when(here)
            def _():
                pltpu.make_async_copy(src, dst, out_sem).start()

            @pl.when(jnp.logical_not(here) & (everyone | (last_row(dest) <= big)))
            def _():
                send(src, dst, out_sem, {"rep": to_rep, "col": to_col})

    def held_output(idx, big, small):
        @pl.when((big % row_size == row) & (small % col_size == col))
        def _():
            pltpu.make_async_copy(
                l_st.at[idx], out_ref.at[big // row_size, small // col_size], out_sem).start()

    deal(0)

    @pl.loop(-1, num - 1)
    def _(i):
        @pl.when((i >= 0) & (i + 1 < cols_blk))
        def _():
            deal(i + 1)

        owner = i % ring
        owner_chip = owner // row_size
        waits = (i >= 0) & (my_last > i) & (owner != me)

        @pl.when(waits)
        def _():
            early = (i % row_size == row) & (owner_chip != chip)

            @pl.loop(jnp.where(early, jnp.maximum(i - NEAR, 0), 0), i)
            def _(j):
                idx = packed(i, j)
                wait_block(l_st.at[idx], l_sem.at[idx])
                held_output(idx, i, j)

        @pl.loop(0, slots)
        def _(s):
            big = me + s * ring
            idx = packed(big, i)
            critical = big == i + 1
            follow = (big < num) & (big > i) & (i >= 0)

            @pl.when(follow)
            def _():
                mine, theirs = packed(big, 0), packed(i, 0)
                acc[...] = jnp.zeros_like(acc)

                @pl.loop(0, i // UNROLL)
                def _(g):
                    base = g * UNROLL
                    acc[...] += tree_sum(
                        [dot_nt(l_st[mine + base + u], l_st[theirs + base + u]) for u in range(UNROLL)])

                @pl.loop(i // UNROLL * UNROLL, i)
                def _(j):
                    acc[...] += dot_nt(l_st[mine + j], l_st[theirs + j])

                wait_block(a_row.at[s, i], a_sem.at[s, i])
                rest = a_row[s, i] - acc[...]

                @pl.when(waits & ((s == 0) | (me <= i)))
                def _():
                    wait_block(w_st.at[i], w_sem.at[i])

                    @pl.when((i % row_size == row) & (owner_chip != chip)
                             & (owner_chip != (chip + chips - 1) % chips))
                    def _():
                        to_partner(w_st.at[i], w_sem.at[i], i)

                l_new = dot_nt(rest, w_st[i])
                l_st[idx] = l_new
                both = jnp.where(big - i <= NEAR, chips, 0)
                to_partner(l_st.at[idx], l_sem.at[idx], big)
                to_chips(l_st.at[idx], l_sem.at[idx], big, 1, jnp.where(critical, 2, chips), both)

                @pl.when(jnp.logical_not(critical))
                def _():
                    own_output(idx, big, i, False)

                d_acc[s] = d_acc[s] + dot_nt(l_new, l_new)

            @pl.when(critical & (big < num))
            def _():
                wait_block(a_row.at[s, big], a_sem.at[s, big])
                acc[...] = a_row[s, big] - d_acc[s]

                def put_u(p, val):
                    u_buf[SUB * p:SUB * p + SUB, :] = val

                def put_w(p, val):
                    w_st[big, SUB * p:SUB * p + SUB, :] = val

                factor_block([acc[SUB * q:SUB * q + SUB, :] for q in range(blk // SUB)], put_u, put_w)
                to_partner(w_st.at[big], w_sem.at[big], big)
                to_chips(w_st.at[big], w_sem.at[big], big, 1, chips, 1)

                @pl.when(follow)
                def _():
                    to_chips(l_st.at[idx], l_sem.at[idx], big, 2, chips, chips)
                    own_output(idx, big, i, False)

                lane = lax.broadcasted_iota(jnp.int32, (blk, blk), 1)
                sub = lax.broadcasted_iota(jnp.int32, (blk, blk), 0)
                diag = packed(big, big)
                l_st[diag] = jnp.where(lane <= sub, u_buf[...].T, 0.0)
                own_output(diag, big, big, True)

        @pl.when(i >= NEAR)
        def _():
            @pl.loop(i + 1, my_last)
            def _(j):
                @pl.when((j % row_size == row) & (j % ring != me))
                def _():
                    idx = packed(j, i - NEAR)
                    wait_block(l_st.at[idx], l_sem.at[idx])
                    to_partner(l_st.at[idx], l_sem.at[idx], j)
                    held_output(idx, j, i - NEAR)

    chunk = 16

    @pl.loop(0, count[0] // chunk)
    def _(t):
        wait_block(l_st.at[0:chunk], send_sem)

    @pl.loop(0, count[0] % chunk)
    def _(t):
        wait_block(l_st.at[0], send_sem)

    wait_block(out_ref, out_sem)


def solution(mesh):
    sizes = tuple(mesh.shape[axis] for axis in ("row", "col", "rep"))
    grid_spec = P(("b", "row"), "col")

    def local_factor(a_loc):
        rows_blk, cols_blk, blk, _ = a_loc.shape
        num = rows_blk * sizes[0]
        ring = sizes[0] * sizes[1] * sizes[2]
        slots = -(-num // ring)
        assert slots <= 2
        f32 = jnp.float32
        dma = pltpu.SemaphoreType.DMA
        tri = num * (num + 1) // 2
        return pl.pallas_call(
            functools.partial(kernel, sizes),
            out_shape=jax.ShapeDtypeStruct(a_loc.shape, f32),
            in_specs=[pl.BlockSpec(memory_space=pl.ANY)],
            out_specs=pl.BlockSpec(memory_space=pl.ANY),
            scratch_shapes=[
                pltpu.VMEM((tri, blk, blk), f32),
                pltpu.VMEM((num, blk, blk), f32),
                pltpu.VMEM((slots, num, blk, blk), f32),
                pltpu.VMEM((slots, blk, blk), f32),
                pltpu.VMEM((blk, blk), f32),
                pltpu.VMEM((blk, blk), f32),
                pltpu.VMEM((blk, blk), f32),
                pltpu.SMEM((1,), jnp.int32),
                dma((tri,)),
                dma((num,)),
                dma((slots, num)),
                dma,
                dma,
            ],
            compiler_params=pltpu.CompilerParams(
                collective_id=0, has_side_effects=True, vmem_limit_bytes=67043328,
            ),
        )(a_loc)

    return jax.shard_map(local_factor, mesh=mesh, in_specs=grid_spec, out_specs=grid_spec, check_vma=False)
```

```python
import functools

import jax
import jax.numpy as jnp
from jax import lax
from jax.experimental import pallas as pl
from jax.experimental.pallas import tpu as pltpu
from jax.sharding import PartitionSpec as P

SUB = 8
NEAR = 2
LAG = 3
UNROLL = 4
MESH = pl.DeviceIdType.MESH


def dot_nt(lhs, rhs):
    return lax.dot_general(
        lhs, rhs, (((1,), (1,)), ((), ())),
        precision=lax.Precision.HIGHEST, preferred_element_type=jnp.float32,
    )


def lane_bcast(vec, lane):
    return jnp.broadcast_to(vec[:, lane:lane + 1], vec.shape)


def sub_bcast(vec, row):
    return jnp.broadcast_to(vec[row:row + 1, :], vec.shape)


def tree_sum(terms):
    while len(terms) > 1:
        terms = [sum(terms[a:a + 2][1:], terms[a]) for a in range(0, len(terms), 2)]
    return terms[0]


def factor_block(mat, put_u, put_w):
    panels = len(mat)
    shape = mat[0].shape
    lane = lax.broadcasted_iota(jnp.int32, shape, 1)
    sub = lax.broadcasted_iota(jnp.int32, shape, 0)
    aug = [jnp.where(lane == sub + SUB * q, 1.0, 0.0).astype(jnp.float32) for q in range(panels)]
    for p in range(panels):
        base = SUB * p
        cols = [lane_bcast(mat[p], base + j) for j in range(SUB)]
        piv = {(i, j): sub_bcast(cols[j], i) for j in range(SUB) for i in range(j, SUB)}
        rows_m = [sub_bcast(mat[p], i) for i in range(SUB)]
        rows_x = [sub_bcast(aug[p], i) for i in range(SUB)]
        low, inv, root = {}, [], []
        for j in range(SUB):
            inv.append(1.0 / piv[j, j])
            root.append(lax.rsqrt(piv[j, j]))
            for i in range(j + 1, SUB):
                low[i, j] = piv[i, j] * inv[j]
            for i in range(j + 1, SUB):
                for k in range(j + 1, i + 1):
                    piv[i, k] = piv[i, k] - low[i, j] * piv[k, j]
                rows_m[i] = rows_m[i] - low[i, j] * rows_m[j]
                rows_x[i] = rows_x[i] - low[i, j] * rows_x[j]
        u_rows = rows_m[0] * root[0]
        w_rows = rows_x[0] * root[0]
        for i in range(1, SUB):
            u_rows = jnp.where(sub == i, rows_m[i] * root[i], u_rows)
            w_rows = jnp.where(sub == i, rows_x[i] * root[i], w_rows)
        put_u(p, u_rows)
        put_w(p, w_rows)
        if p + 1 == panels:
            break
        back_m = [rows_m[i] * inv[i] for i in range(SUB)]
        back_x = [rows_x[i] * inv[i] for i in range(SUB)]
        for i in range(SUB - 2, -1, -1):
            for j in range(SUB - 1, i, -1):
                back_m[i] = back_m[i] - low[j, i] * back_m[j]
                back_x[i] = back_x[i] - low[j, i] * back_x[j]
        for q in range(p + 1, panels):
            coef = [lane_bcast(mat[q], base + j) for j in range(SUB)]
            mat[q] = mat[q] - tree_sum([coef[j] * back_m[j] for j in range(SUB)])
            aug[q] = aug[q] - tree_sum([coef[j] * back_x[j] for j in range(SUB)])


def kernel(sizes, a_ref, out_ref, l_st, w_st, a_row, d_acc, acc, u_buf, zero_buf, count,
           l_sem, w_sem, a_sem, out_sem, send_sem):
    row_size, col_size, rep_size = sizes
    rows_blk, cols_blk, blk, _ = a_ref.shape
    num = rows_blk * row_size
    chips = col_size * rep_size
    ring = chips * row_size
    slots = a_row.shape[0]
    twin = max(num - ring, 0)
    row, col, rep = lax.axis_index("row"), lax.axis_index("col"), lax.axis_index("rep")

    def snake(y, x):
        return jnp.where(y % 2 == 0, x, col_size - 1 - x)

    chip = rep * col_size + snake(rep, col)
    me = chip * row_size + row

    def place(other_chip, other_row):
        y = other_chip // col_size
        return {"rep": y, "col": snake(y, other_chip % col_size), "row": other_row}

    def last_row(dev):
        return jnp.where(dev >= ring - twin, dev + twin, dev)

    def chip_at(y, x):
        return y * col_size + snake(y, x)

    def chip_last(other_chip):
        return last_row(other_chip * row_size + row_size - 1)

    def owner_of(big):
        return jnp.where(big >= ring, big - twin, big)

    my_last = last_row(me)
    x_first = row == 0

    def packed(big, small):
        return (big * (big + 1)) // 2 + small

    def send(src, dst, sem, where):
        count[0] = count[0] + 1
        pltpu.make_async_remote_copy(
            src_ref=src, dst_ref=dst, send_sem=send_sem, recv_sem=sem,
            device_id=where, device_id_type=MESH,
        ).start()

    def wait_block(ref, sem):
        pltpu.make_async_copy(ref, ref, sem).wait()

    barrier = pltpu.get_barrier_semaphore()

    @pl.loop(1, ring)
    def _(t):
        dev = (me + t) % ring
        pl.semaphore_signal(
            barrier, inc=1, device_id=place(dev // row_size, dev % row_size), device_id_type=MESH)

    count[0] = 0
    zero_buf[...] = jnp.zeros_like(zero_buf)
    d_acc[...] = jnp.zeros_like(d_acc)

    @pl.loop(0, rows_blk)
    def _(i):
        @pl.loop(0, cols_blk)
        def _(j):
            @pl.when(j * col_size + col > i * row_size + row)
            def _():
                pltpu.make_async_copy(zero_buf, out_ref.at[i, j], out_sem).start()

    pl.semaphore_wait(barrier, ring - 1)

    def deal(jj):
        j = jj * col_size + col
        for to_col in range(col_size):
            for s in range(slots):
                dev = chip_at(rep, to_col) * row_size + row
                big = dev + s * twin
                real = j <= big
                if s:
                    real = real & (dev >= ring - twin)

                @pl.when(real)
                def _():
                    src, dst = a_ref.at[big // row_size, jj], a_row.at[s, j]

                    @pl.when(col == to_col)
                    def _():
                        pltpu.make_async_copy(src, dst, a_sem.at[s, j]).start()

                    @pl.when(col != to_col)
                    def _():
                        send(src, dst, a_sem.at[s, j], {"col": to_col})

    def to_partner(ref, sem, big):
        for other in range(row_size):
            @pl.when((row != other) & (last_row(chip * row_size + other) > big))
            def _():
                send(ref, ref, sem, {"row": other})

    def to_chips(ref, sem, big, lo, hi, both):
        @pl.loop(lo, hi)
        def _(t):
            dest = (chip + t) % chips
            for shift in range(row_size):
                core = (row + row_size - 1 - shift) % row_size
                wanted = last_row(dest * row_size + core) > big
                if shift < row_size - 1:
                    wanted = wanted & (t <= both)

                @pl.when(wanted)
                def _():
                    send(ref, ref, sem, place(dest, core))

    def to_col_peers(ref, sem, big, whole):
        for shift in range(1, col_size):
            x = (col + shift) % col_size
            wanted = chip_last(chip_at(jnp.where(whole, rep_size - 1, rep), x)) > big

            @pl.when(wanted)
            def _():
                send(ref, ref, sem, {"col": x})

    def to_rep_peers(ref, sem, big, whole):
        for shift in range(1, rep_size):
            y = (rep + shift) % rep_size
            wanted = jnp.where(whole, chip_last(y * col_size + col_size - 1), chip_last(chip_at(y, col))) > big

            @pl.when(wanted)
            def _():
                send(ref, ref, sem, {"rep": y})

    def arrived(idx, big, small):
        to_partner(l_st.at[idx], l_sem.at[idx], big)

        @pl.when(my_last > big)
        def _():
            held_output(idx, big, small)

    def passed_down(small):
        return small < num - 1 - LAG - rep_size

    def reaches(big, small, x):
        there = chip_at(rep, x)
        relays = x_first & (big - small > NEAR) & (chip_last(chip_at(rep_size - 1, x)) > big)
        return (last_row(there * row_size + row) > big) | relays

    def own_output(idx, big, small, diagonal):
        src, dst = l_st.at[idx], out_ref.at[big // row_size, small // col_size]
        to_col = small % col_size
        down = passed_down(small) & (big != small)

        @pl.when(to_col == col)
        def _():
            pltpu.make_async_copy(src, dst, out_sem).start()

        @pl.when(down & (to_col != col) & jnp.logical_not(reaches(big, small, to_col)))
        def _():
            send(src, src, l_sem.at[idx], {"col": to_col})

        @pl.when(jnp.logical_not(down))
        def _():
            for to_rep in range(rep_size):
                dest = chip_at(jnp.int32(to_rep), to_col) * row_size + row

                @pl.when((dest != me) & (diagonal | (last_row(dest) <= big)))
                def _():
                    send(src, dst, out_sem, {"rep": to_rep, "col": to_col})

    def held_output(idx, big, small):
        @pl.when((big % row_size == row) & (small % col_size == col))
        def _():
            pltpu.make_async_copy(
                l_st.at[idx], out_ref.at[big // row_size, small // col_size], out_sem).start()

    deal(0)

    @pl.loop(-1, num - 1)
    def _(i):
        @pl.when((i >= 0) & (i + 1 < cols_blk))
        def _():
            deal(i + 1)

        owner = owner_of(i)
        owner_chip = owner // row_size
        waits = (i >= 0) & (my_last > i) & (owner != me)

        @pl.when(waits)
        def _():
            early = (i % row_size == row) & (owner_chip != chip)

            @pl.loop(jnp.where(early, jnp.maximum(i - NEAR, 0), 0), i)
            def _(j):
                idx = packed(i, j)
                wait_block(l_st.at[idx], l_sem.at[idx])

                @pl.when(early & (owner_chip != (chip + chips - 1) % chips))
                def _():
                    to_partner(l_st.at[idx], l_sem.at[idx], i)

                held_output(idx, i, j)

        @pl.loop(0, slots)
        def _(s):
            big = me + s * twin
            idx = packed(big, i)
            real = (s == 0) | (me >= ring - twin)
            critical = real & (big == i + 1)
            follow = real & (big > i) & (i >= 0)

            @pl.when(follow)
            def _():
                mine, theirs = packed(big, 0), packed(i, 0)
                acc[...] = jnp.zeros_like(acc)

                @pl.loop(0, i // UNROLL)
                def _(g):
                    base = g * UNROLL
                    acc[...] += dot_nt(
                        jnp.concatenate([l_st[mine + base + u] for u in range(UNROLL)], axis=1),
                        jnp.concatenate([l_st[theirs + base + u] for u in range(UNROLL)], axis=1))

                @pl.loop(i // UNROLL * UNROLL, i)
                def _(j):
                    acc[...] += dot_nt(l_st[mine + j], l_st[theirs + j])

                wait_block(a_row.at[s, i], a_sem.at[s, i])
                rest = a_row[s, i] - acc[...]

                @pl.when(waits & ((s == 0) | (me <= i)))
                def _():
                    wait_block(w_st.at[i], w_sem.at[i])

                    @pl.when((i % row_size == row) & (owner_chip != chip)
                             & (owner_chip != (chip + chips - 1) % chips))
                    def _():
                        to_partner(w_st.at[i], w_sem.at[i], i)

                l_new = dot_nt(rest, w_st[i])
                l_st[idx] = l_new
                new, new_sem = l_st.at[idx], l_sem.at[idx]
                near = big - i <= NEAR
                to_partner(new, new_sem, big)

                @pl.when(near)
                def _():
                    to_chips(new, new_sem, big, 1, jnp.where(critical, 2, chips), 1)

                @pl.when(jnp.logical_not(near))
                def _():
                    to_col_peers(new, new_sem, big, x_first)
                    to_rep_peers(new, new_sem, big, jnp.logical_not(x_first))

                @pl.when(jnp.logical_not(critical))
                def _():
                    own_output(idx, big, i, False)

                d_acc[s] = d_acc[s] + dot_nt(l_new, l_new)

            @pl.when(critical)
            def _():
                wait_block(a_row.at[s, big], a_sem.at[s, big])
                acc[...] = a_row[s, big] - d_acc[s]

                def put_u(p, val):
                    u_buf[SUB * p:SUB * p + SUB, :] = val

                def put_w(p, val):
                    w_st[big, SUB * p:SUB * p + SUB, :] = val

                factor_block([acc[SUB * q:SUB * q + SUB, :] for q in range(blk // SUB)], put_u, put_w)
                to_partner(w_st.at[big], w_sem.at[big], big)
                to_chips(w_st.at[big], w_sem.at[big], big, 1, chips, 1)

                @pl.when(follow)
                def _():
                    to_chips(l_st.at[idx], l_sem.at[idx], big, 2, chips, 1)
                    own_output(idx, big, i, False)

                lane = lax.broadcasted_iota(jnp.int32, (blk, blk), 1)
                sub = lax.broadcasted_iota(jnp.int32, (blk, blk), 0)
                diag = packed(big, big)
                l_st[diag] = jnp.where(lane <= sub, u_buf[...].T, 0.0)
                own_output(diag, big, big, True)

        def relay(source, along):
            for s in range(slots):
                big = source + s * twin
                real = big - i >= NEAR
                if s:
                    real = real & (source >= ring - twin)
                if along == "rep":
                    real = real & (chip_last(chip_at(rep_size - 1, col)) > big)
                else:
                    real = real & (chip_last(rep * col_size + col_size - 1) > big)

                @pl.when(real)
                def _():
                    idx = packed(big, i - 1)
                    wait_block(l_st.at[idx], l_sem.at[idx])
                    if along == "rep":
                        to_rep_peers(l_st.at[idx], l_sem.at[idx], big, False)
                    else:
                        to_col_peers(l_st.at[idx], l_sem.at[idx], big, False)
                    arrived(idx, big, i - 1)

        @pl.when((i >= 1) & x_first)
        def _():
            for shift in range(1, col_size):
                relay(chip_at(rep, (col + shift) % col_size) * row_size + row, "rep")

        @pl.when((i >= 1) & jnp.logical_not(x_first))
        def _():
            for shift in range(1, rep_size):
                relay(chip_at((rep + shift) % rep_size, col) * row_size + row, "col")

        @pl.when(i >= NEAR)
        def _():
            @pl.loop(i + 1, my_last)
            def _(j):
                source = owner_of(j) // row_size
                y = source // col_size
                second = jnp.where(x_first, y != rep, snake(y, source % col_size) != col)

                @pl.when((j % row_size == row) & second)
                def _():
                    idx = packed(j, i - NEAR)
                    wait_block(l_st.at[idx], l_sem.at[idx])
                    arrived(idx, j, i - NEAR)

        @pl.loop(0, rep_size)
        def _(gap):
            small = i - LAG - gap
            y = rep + gap

            @pl.when((small >= 0) & (small % col_size == col) & (y < rep_size) & passed_down(small))
            def _():
                @pl.loop(0, col_size)
                def _(x):
                    dev = chip_at(y, x) * row_size + row

                    for s in range(slots):
                        big = dev + s * twin
                        real = big > small
                        if s:
                            real = real & (dev >= ring - twin)

                        @pl.when(real)
                        def _():
                            idx = packed(big, small)
                            held = (gap == 0) & ((dev == me) | (my_last > big))

                            @pl.when(jnp.where(gap == 0, (dev != me) & jnp.logical_not(reaches(big, small, col)), True))
                            def _():
                                wait_block(l_st.at[idx], l_sem.at[idx])

                            @pl.when(jnp.logical_not(held))
                            def _():
                                held_output(idx, big, small)

                            @pl.when(rep > 0)
                            def _():
                                send(l_st.at[idx], l_st.at[idx], l_sem.at[idx], {"rep": rep - 1})

    chunk = 16

    @pl.loop(0, count[0] // chunk)
    def _(t):
        wait_block(l_st.at[0:chunk], send_sem)

    @pl.loop(0, count[0] % chunk)
    def _(t):
        wait_block(l_st.at[0], send_sem)

    wait_block(out_ref, out_sem)


def solution(mesh):
    sizes = tuple(mesh.shape[axis] for axis in ("row", "col", "rep"))
    grid_spec = P(("b", "row"), "col")

    def local_factor(a_loc):
        rows_blk, cols_blk, blk, _ = a_loc.shape
        num = rows_blk * sizes[0]
        ring = sizes[0] * sizes[1] * sizes[2]
        slots = -(-num // ring)
        assert slots <= 2
        f32 = jnp.float32
        dma = pltpu.SemaphoreType.DMA
        tri = num * (num + 1) // 2
        return pl.pallas_call(
            functools.partial(kernel, sizes),
            out_shape=jax.ShapeDtypeStruct(a_loc.shape, f32),
            in_specs=[pl.BlockSpec(memory_space=pl.ANY)],
            out_specs=pl.BlockSpec(memory_space=pl.ANY),
            scratch_shapes=[
                pltpu.VMEM((tri, blk, blk), f32),
                pltpu.VMEM((num, blk, blk), f32),
                pltpu.VMEM((slots, num, blk, blk), f32),
                pltpu.VMEM((slots, blk, blk), f32),
                pltpu.VMEM((blk, blk), f32),
                pltpu.VMEM((blk, blk), f32),
                pltpu.VMEM((blk, blk), f32),
                pltpu.SMEM((1,), jnp.int32),
                dma((tri,)),
                dma((num,)),
                dma((slots, num)),
                dma,
                dma,
            ],
            compiler_params=pltpu.CompilerParams(
                collective_id=0, has_side_effects=True, vmem_limit_bytes=67043328,
            ),
        )(a_loc)

    return jax.shard_map(local_factor, mesh=mesh, in_specs=grid_spec, out_specs=grid_spec, check_vma=False)
```

```python
import functools

import jax
import jax.numpy as jnp
from jax import lax
from jax.experimental import pallas as pl
from jax.experimental.pallas import tpu as pltpu
from jax.sharding import PartitionSpec as P

SUB = 8
NEAR = 2
LAG = 3
UNROLL = 4
MESH = pl.DeviceIdType.MESH


def dot_nt(lhs, rhs):
    return lax.dot_general(
        lhs, rhs, (((1,), (1,)), ((), ())),
        precision=lax.Precision.HIGHEST, preferred_element_type=jnp.float32,
    )


def lane_bcast(vec, lane):
    return jnp.broadcast_to(vec[:, lane:lane + 1], vec.shape)


def sub_bcast(vec, row):
    return jnp.broadcast_to(vec[row:row + 1, :], vec.shape)


def tree_sum(terms):
    while len(terms) > 1:
        terms = [sum(terms[a:a + 2][1:], terms[a]) for a in range(0, len(terms), 2)]
    return terms[0]


def factor_block(mat, put_u, put_w):
    panels = len(mat)
    shape = mat[0].shape
    lane = lax.broadcasted_iota(jnp.int32, shape, 1)
    sub = lax.broadcasted_iota(jnp.int32, shape, 0)
    aug = [jnp.where(lane == sub + SUB * q, 1.0, 0.0).astype(jnp.float32) for q in range(panels)]
    for p in range(panels):
        base = SUB * p
        cols = [lane_bcast(mat[p], base + j) for j in range(SUB)]
        piv = {(i, j): sub_bcast(cols[j], i) for j in range(SUB) for i in range(j, SUB)}
        rows_m = [sub_bcast(mat[p], i) for i in range(SUB)]
        rows_x = [sub_bcast(aug[p], i) for i in range(SUB)]
        low, inv, root = {}, [], []
        for j in range(SUB):
            inv.append(1.0 / piv[j, j])
            root.append(lax.rsqrt(piv[j, j]))
            for i in range(j + 1, SUB):
                low[i, j] = piv[i, j] * inv[j]
            for i in range(j + 1, SUB):
                for k in range(j + 1, i + 1):
                    piv[i, k] = piv[i, k] - low[i, j] * piv[k, j]
                rows_m[i] = rows_m[i] - low[i, j] * rows_m[j]
                rows_x[i] = rows_x[i] - low[i, j] * rows_x[j]
        u_rows = rows_m[0] * root[0]
        w_rows = rows_x[0] * root[0]
        for i in range(1, SUB):
            u_rows = jnp.where(sub == i, rows_m[i] * root[i], u_rows)
            w_rows = jnp.where(sub == i, rows_x[i] * root[i], w_rows)
        put_u(p, u_rows)
        put_w(p, w_rows)
        if p + 1 == panels:
            break
        back_m = [rows_m[i] * inv[i] for i in range(SUB)]
        back_x = [rows_x[i] * inv[i] for i in range(SUB)]
        for i in range(SUB - 2, -1, -1):
            for j in range(SUB - 1, i, -1):
                back_m[i] = back_m[i] - low[j, i] * back_m[j]
                back_x[i] = back_x[i] - low[j, i] * back_x[j]
        for q in range(p + 1, panels):
            coef = [lane_bcast(mat[q], base + j) for j in range(SUB)]
            mat[q] = mat[q] - tree_sum([coef[j] * back_m[j] for j in range(SUB)])
            aug[q] = aug[q] - tree_sum([coef[j] * back_x[j] for j in range(SUB)])


def div(num, den):
    return lax.div(num, jnp.int32(den))


def rem(num, den):
    return lax.rem(num, jnp.int32(den))


def kernel(sizes, a_ref, out_ref, l_st, w_st, a_row, d_acc, acc, u_buf, zero_buf, count,
           l_sem, w_sem, a_sem, out_sem, send_sem):
    row_size, col_size, rep_size = sizes
    rows_blk, cols_blk, blk, _ = a_ref.shape
    num = rows_blk * row_size
    chips = col_size * rep_size
    ring = chips * row_size
    slots = a_row.shape[0]
    twin = max(num - ring, 0)
    row, col, rep = lax.axis_index("row"), lax.axis_index("col"), lax.axis_index("rep")

    def snake(y, x):
        return jnp.where(rem(y, 2) == 0, x, col_size - 1 - x)

    chip = rep * col_size + snake(rep, col)
    me = chip * row_size + row

    def place(other_chip, other_row):
        y = div(other_chip, col_size)
        return {"rep": y, "col": snake(y, other_chip - y * col_size), "row": other_row}

    def last_row(dev):
        return jnp.where(dev >= ring - twin, dev + twin, dev)

    def chip_at(y, x):
        return y * col_size + snake(y, x)

    def chip_last(other_chip):
        return last_row(other_chip * row_size + row_size - 1)

    def owner_of(big):
        return jnp.where(big >= ring, big - twin, big)

    my_last = last_row(me)
    x_first = row == 0

    def packed(big, small):
        return div(big * (big + 1), 2) + small

    def send(src, dst, sem, where):
        count[0] = count[0] + 1
        pltpu.make_async_remote_copy(
            src_ref=src, dst_ref=dst, send_sem=send_sem, recv_sem=sem,
            device_id=where, device_id_type=MESH,
        ).start()

    def wait_block(ref, sem):
        pltpu.make_async_copy(ref, ref, sem).wait()

    barrier = pltpu.get_barrier_semaphore()

    @pl.loop(1, ring)
    def _(t):
        dev = rem(me + t, ring)
        pl.semaphore_signal(
            barrier, inc=1, device_id=place(div(dev, row_size), rem(dev, row_size)), device_id_type=MESH)

    count[0] = 0
    zero_buf[...] = jnp.zeros_like(zero_buf)
    d_acc[...] = jnp.zeros_like(d_acc)

    @pl.loop(0, rows_blk)
    def _(i):
        @pl.loop(0, cols_blk)
        def _(j):
            @pl.when(j * col_size + col > i * row_size + row)
            def _():
                pltpu.make_async_copy(zero_buf, out_ref.at[i, j], out_sem).start()

    pl.semaphore_wait(barrier, ring - 1)

    def deal(jj):
        j = jj * col_size + col
        for to_col in range(col_size):
            for s in range(slots):
                dev = chip_at(rep, to_col) * row_size + row
                big = dev + s * twin
                real = j <= big
                if s:
                    real = real & (dev >= ring - twin)

                @pl.when(real)
                def _():
                    src, dst = a_ref.at[div(big, row_size), jj], a_row.at[s, j]

                    @pl.when(col == to_col)
                    def _():
                        pltpu.make_async_copy(src, dst, a_sem.at[s, j]).start()

                    @pl.when(col != to_col)
                    def _():
                        send(src, dst, a_sem.at[s, j], {"col": to_col})

    def to_partner(ref, sem, big):
        for other in range(row_size):
            @pl.when((row != other) & (last_row(chip * row_size + other) > big))
            def _():
                send(ref, ref, sem, {"row": other})

    def to_chips(ref, sem, big, lo, hi, both):
        @pl.loop(lo, hi)
        def _(t):
            dest = rem(chip + t, chips)
            for shift in range(row_size):
                core = rem(row + row_size - 1 - shift, row_size)
                wanted = last_row(dest * row_size + core) > big
                if shift < row_size - 1:
                    wanted = wanted & (t <= both)

                @pl.when(wanted)
                def _():
                    send(ref, ref, sem, place(dest, core))

    def to_col_peers(ref, sem, big, whole):
        for shift in range(1, col_size):
            x = rem(col + shift, col_size)
            wanted = chip_last(chip_at(jnp.where(whole, rep_size - 1, rep), x)) > big

            @pl.when(wanted)
            def _():
                send(ref, ref, sem, {"col": x})

    def to_rep_peers(ref, sem, big, whole):
        for shift in range(1, rep_size):
            y = rem(rep + shift, rep_size)
            wanted = jnp.where(whole, chip_last(y * col_size + col_size - 1), chip_last(chip_at(y, col))) > big

            @pl.when(wanted)
            def _():
                send(ref, ref, sem, {"rep": y})

    def arrived(idx, big, small):
        to_partner(l_st.at[idx], l_sem.at[idx], big)

        @pl.when(my_last > big)
        def _():
            held_output(idx, big, small)

    def passed_down(small):
        return small < num - 1 - LAG - rep_size

    def reaches(big, small, x):
        there = chip_at(rep, x)
        relays = x_first & (big - small > NEAR) & (chip_last(chip_at(rep_size - 1, x)) > big)
        return (last_row(there * row_size + row) > big) | relays

    def own_output(idx, big, small, diagonal):
        src, dst = l_st.at[idx], out_ref.at[div(big, row_size), div(small, col_size)]
        to_col = rem(small, col_size)
        down = passed_down(small) & (big != small)

        @pl.when(to_col == col)
        def _():
            pltpu.make_async_copy(src, dst, out_sem).start()

        @pl.when(down & (to_col != col) & jnp.logical_not(reaches(big, small, to_col)))
        def _():
            send(src, src, l_sem.at[idx], {"col": to_col})

        @pl.when(jnp.logical_not(down))
        def _():
            for to_rep in range(rep_size):
                dest = chip_at(jnp.int32(to_rep), to_col) * row_size + row

                @pl.when((dest != me) & (diagonal | (last_row(dest) <= big)))
                def _():
                    send(src, dst, out_sem, {"rep": to_rep, "col": to_col})

    def held_output(idx, big, small):
        @pl.when((rem(big, row_size) == row) & (rem(small, col_size) == col))
        def _():
            pltpu.make_async_copy(
                l_st.at[idx], out_ref.at[div(big, row_size), div(small, col_size)], out_sem).start()

    deal(0)
    deal(1)

    @pl.loop(-1, num - 1)
    def _(i):
        @pl.when((i >= 0) & (rem(i, col_size) == 0) & (div(i, col_size) + 2 < cols_blk))
        def _():
            deal(div(i, col_size) + 2)

        owner = owner_of(i)
        owner_chip = div(owner, row_size)
        before = owner_chip == rem(chip + chips - 1, chips)
        same_core = rem(i, row_size) == row
        waits = (i >= 0) & (my_last > i) & (owner != me)

        far = jnp.maximum(i - NEAR, 0)
        theirs = packed(i, 0)

        @pl.when(waits & jnp.logical_not(same_core & (owner_chip != chip)))
        def _():
            @pl.loop(0, far)
            def _(j):
                wait_block(l_st.at[theirs + j], l_sem.at[theirs + j])

        def wait_near():
            @pl.loop(far, i)
            def _(j):
                idx = theirs + j
                wait_block(l_st.at[idx], l_sem.at[idx])

                @pl.when(same_core & (owner_chip != chip))
                def _():
                    @pl.when(jnp.logical_not(before))
                    def _():
                        to_partner(l_st.at[idx], l_sem.at[idx], i)

                    held_output(idx, i, j)

        @pl.loop(0, slots)
        def _(s):
            big = me + s * twin
            idx = packed(big, i)
            real = (s == 0) | (me >= ring - twin)
            critical = real & (big == i + 1)
            follow = real & (big > i) & (i >= 0)

            @pl.when(follow)
            def _():
                mine = packed(big, 0)
                first_slot = (s == 0) | (me <= i)
                acc[...] = jnp.zeros_like(acc)
                quads = div(far, UNROLL)

                @pl.loop(0, quads)
                def _(g):
                    base = g * UNROLL
                    acc[...] += dot_nt(
                        jnp.concatenate([l_st[mine + base + u] for u in range(UNROLL)], axis=1),
                        jnp.concatenate([l_st[theirs + base + u] for u in range(UNROLL)], axis=1))

                @pl.when(waits & first_slot)
                def _():
                    wait_near()

                @pl.loop(quads, div(i + UNROLL - 1, UNROLL))
                def _(g):
                    base = g * UNROLL
                    last = [jnp.minimum(base + u, i - 1) for u in range(UNROLL)]
                    acc[...] += dot_nt(
                        jnp.concatenate([jnp.where(base + u < i, l_st[mine + last[u]], 0.0) for u in range(UNROLL)], axis=1),
                        jnp.concatenate([l_st[theirs + last[u]] for u in range(UNROLL)], axis=1))

                wait_block(a_row.at[s, i], a_sem.at[s, i])
                rest = a_row[s, i] - acc[...]

                @pl.when(waits & first_slot)
                def _():
                    wait_block(w_st.at[i], w_sem.at[i])

                    @pl.when(same_core & (owner_chip != chip) & jnp.logical_not(before))
                    def _():
                        to_partner(w_st.at[i], w_sem.at[i], i)

                l_new = dot_nt(rest, w_st[i])
                l_st[idx] = l_new
                new, new_sem = l_st.at[idx], l_sem.at[idx]
                near = big - i <= NEAR
                to_partner(new, new_sem, big)

                @pl.when(near)
                def _():
                    to_chips(new, new_sem, big, 1, jnp.where(critical, 2, chips), 1)

                @pl.when(jnp.logical_not(near))
                def _():
                    to_col_peers(new, new_sem, big, x_first)
                    to_rep_peers(new, new_sem, big, jnp.logical_not(x_first))

                @pl.when(jnp.logical_not(critical))
                def _():
                    own_output(idx, big, i, False)

                d_acc[s] = d_acc[s] + dot_nt(l_new, l_new)

            @pl.when(critical)
            def _():
                wait_block(a_row.at[s, big], a_sem.at[s, big])
                acc[...] = a_row[s, big] - d_acc[s]

                def put_u(p, val):
                    u_buf[SUB * p:SUB * p + SUB, :] = val

                def put_w(p, val):
                    w_st[big, SUB * p:SUB * p + SUB, :] = val

                factor_block([acc[SUB * q:SUB * q + SUB, :] for q in range(blk // SUB)], put_u, put_w)
                to_partner(w_st.at[big], w_sem.at[big], big)
                to_chips(w_st.at[big], w_sem.at[big], big, 1, chips, 1)

                @pl.when(follow)
                def _():
                    to_chips(l_st.at[idx], l_sem.at[idx], big, 2, chips, 1)
                    own_output(idx, big, i, False)

                lane = lax.broadcasted_iota(jnp.int32, (blk, blk), 1)
                sub = lax.broadcasted_iota(jnp.int32, (blk, blk), 0)
                diag = packed(big, big)
                l_st[diag] = jnp.where(lane <= sub, u_buf[...].T, 0.0)
                own_output(diag, big, big, True)

        soon = (me == i + 2) | ((me >= ring - twin) & (me + twin == i + 2))
        now = (me == i + 1) | ((me >= ring - twin) & (me + twin == i + 1))

        @pl.loop(jnp.where(now, jnp.maximum(i - 1, -1), i), jnp.where(soon, i, i + 1))
        def _(q):
            def relay(source, along):
                for s in range(slots):
                    big = source + s * twin
                    real = big - q >= NEAR
                    if s:
                        real = real & (source >= ring - twin)
                    if along == "rep":
                        real = real & (chip_last(chip_at(rep_size - 1, col)) > big)
                    else:
                        real = real & (chip_last(rep * col_size + col_size - 1) > big)

                    @pl.when(real)
                    def _():
                        idx = packed(big, q - 1)
                        wait_block(l_st.at[idx], l_sem.at[idx])
                        if along == "rep":
                            to_rep_peers(l_st.at[idx], l_sem.at[idx], big, False)
                        else:
                            to_col_peers(l_st.at[idx], l_sem.at[idx], big, False)
                        arrived(idx, big, q - 1)

            @pl.when((q >= 1) & x_first)
            def _():
                for shift in range(1, col_size):
                    relay(chip_at(rep, rem(col + shift, col_size)) * row_size + row, "rep")

            @pl.when((q >= 1) & jnp.logical_not(x_first))
            def _():
                for shift in range(1, rep_size):
                    relay(chip_at(rem(rep + shift, rep_size), col) * row_size + row, "col")

            @pl.when(q >= NEAR)
            def _():
                first = q + 1 + rem(q + 1 + row, row_size)

                @pl.loop(0, div(jnp.maximum(my_last - first, 0) + row_size - 1, row_size))
                def _(t):
                    j = first + t * row_size
                    source = div(owner_of(j), row_size)
                    y = div(source, col_size)
                    second = jnp.where(x_first, y != rep, snake(y, source - y * col_size) != col)

                    @pl.when(second)
                    def _():
                        idx = packed(j, q - NEAR)
                        wait_block(l_st.at[idx], l_sem.at[idx])
                        arrived(idx, j, q - NEAR)

            @pl.loop(0, rep_size)
            def _(gap):
                small = q - LAG - gap
                y = rep + gap

                @pl.when((small >= 0) & (rem(jnp.maximum(small, 0), col_size) == col) & (y < rep_size) & passed_down(small))
                def _():
                    @pl.loop(0, col_size)
                    def _(x):
                        dev = chip_at(y, x) * row_size + row

                        for s in range(slots):
                            big = dev + s * twin
                            real = big > small
                            if s:
                                real = real & (dev >= ring - twin)

                            @pl.when(real)
                            def _():
                                idx = packed(big, small)
                                held = (gap == 0) & ((dev == me) | (my_last > big))

                                @pl.when(jnp.where(gap == 0, (dev != me) & jnp.logical_not(reaches(big, small, col)), True))
                                def _():
                                    wait_block(l_st.at[idx], l_sem.at[idx])

                                @pl.when(jnp.logical_not(held))
                                def _():
                                    held_output(idx, big, small)

                                @pl.when(rep > 0)
                                def _():
                                    send(l_st.at[idx], l_st.at[idx], l_sem.at[idx], {"rep": rep - 1})

    chunk = 16

    @pl.loop(0, div(count[0], chunk))
    def _(t):
        wait_block(l_st.at[0:chunk], send_sem)

    @pl.loop(0, rem(count[0], chunk))
    def _(t):
        wait_block(l_st.at[0], send_sem)

    wait_block(out_ref, out_sem)


def solution(mesh):
    sizes = tuple(mesh.shape[axis] for axis in ("row", "col", "rep"))
    grid_spec = P(("b", "row"), "col")

    def local_factor(a_loc):
        rows_blk, cols_blk, blk, _ = a_loc.shape
        num = rows_blk * sizes[0]
        ring = sizes[0] * sizes[1] * sizes[2]
        slots = -(-num // ring)
        assert slots <= 2
        f32 = jnp.float32
        dma = pltpu.SemaphoreType.DMA
        tri = num * (num + 1) // 2
        return pl.pallas_call(
            functools.partial(kernel, sizes),
            out_shape=jax.ShapeDtypeStruct(a_loc.shape, f32),
            in_specs=[pl.BlockSpec(memory_space=pl.ANY)],
            out_specs=pl.BlockSpec(memory_space=pl.ANY),
            scratch_shapes=[
                pltpu.VMEM((tri, blk, blk), f32),
                pltpu.VMEM((num, blk, blk), f32),
                pltpu.VMEM((slots, num, blk, blk), f32),
                pltpu.VMEM((slots, blk, blk), f32),
                pltpu.VMEM((blk, blk), f32),
                pltpu.VMEM((blk, blk), f32),
                pltpu.VMEM((blk, blk), f32),
                pltpu.SMEM((1,), jnp.int32),
                dma((tri,)),
                dma((num,)),
                dma((slots, num)),
                dma,
                dma,
            ],
            compiler_params=pltpu.CompilerParams(
                collective_id=0, has_side_effects=True, vmem_limit_bytes=67043328,
            ),
        )(a_loc)

    return jax.shard_map(local_factor, mesh=mesh, in_specs=grid_spec, out_specs=grid_spec, check_vma=False)
```

```python
import functools

import jax
import jax.numpy as jnp
from jax import lax
from jax.experimental import pallas as pl
from jax.experimental.pallas import tpu as pltpu
from jax.sharding import PartitionSpec as P

SUB = 8
NEAR = 2
LAG = 3
UNROLL = 4
MESH = pl.DeviceIdType.MESH


def dot_nt(lhs, rhs):
    return lax.dot_general(
        lhs, rhs, (((1,), (1,)), ((), ())),
        precision=lax.Precision.HIGHEST, preferred_element_type=jnp.float32,
    )


def lane_bcast(vec, lane):
    return jnp.broadcast_to(vec[:, lane:lane + 1], vec.shape)


def sub_bcast(vec, row):
    return jnp.broadcast_to(vec[row:row + 1, :], vec.shape)


def tree_sum(terms):
    while len(terms) > 1:
        terms = [sum(terms[a:a + 2][1:], terms[a]) for a in range(0, len(terms), 2)]
    return terms[0]


def factor_block(mat, put_u, put_w):
    panels = len(mat)
    shape = mat[0].shape
    lane = lax.broadcasted_iota(jnp.int32, shape, 1)
    sub = lax.broadcasted_iota(jnp.int32, shape, 0)
    aug = [jnp.where(lane == sub + SUB * q, 1.0, 0.0).astype(jnp.float32) for q in range(panels)]
    for p in range(panels):
        base = SUB * p
        cols = [lane_bcast(mat[p], base + j) for j in range(SUB)]
        piv = {(i, j): sub_bcast(cols[j], i) for j in range(SUB) for i in range(j, SUB)}
        rows_m = [sub_bcast(mat[p], i) for i in range(SUB)]
        rows_x = [sub_bcast(aug[p], i) for i in range(SUB)]
        low, inv, root = {}, [], []
        for j in range(SUB):
            inv.append(1.0 / piv[j, j])
            root.append(lax.rsqrt(piv[j, j]))
            for i in range(j + 1, SUB):
                low[i, j] = piv[i, j] * inv[j]
            for i in range(j + 1, SUB):
                for k in range(j + 1, i + 1):
                    piv[i, k] = piv[i, k] - low[i, j] * piv[k, j]
                rows_m[i] = rows_m[i] - low[i, j] * rows_m[j]
                rows_x[i] = rows_x[i] - low[i, j] * rows_x[j]
        u_rows = rows_m[0] * root[0]
        w_rows = rows_x[0] * root[0]
        for i in range(1, SUB):
            u_rows = jnp.where(sub == i, rows_m[i] * root[i], u_rows)
            w_rows = jnp.where(sub == i, rows_x[i] * root[i], w_rows)
        put_u(p, u_rows)
        put_w(p, w_rows)
        if p + 1 == panels:
            break
        back_m = [rows_m[i] * inv[i] for i in range(SUB)]
        back_x = [rows_x[i] * inv[i] for i in range(SUB)]
        for i in range(SUB - 2, -1, -1):
            for j in range(SUB - 1, i, -1):
                back_m[i] = back_m[i] - low[j, i] * back_m[j]
                back_x[i] = back_x[i] - low[j, i] * back_x[j]
        for q in range(p + 1, panels):
            coef = [lane_bcast(mat[q], base + j) for j in range(SUB)]
            mat[q] = mat[q] - tree_sum([coef[j] * back_m[j] for j in range(SUB)])
            aug[q] = aug[q] - tree_sum([coef[j] * back_x[j] for j in range(SUB)])


def div(num, den):
    return lax.div(num, jnp.int32(den))


def rem(num, den):
    return lax.rem(num, jnp.int32(den))


def kernel(sizes, a_ref, out_ref, l_st, w_st, a_row, d_acc, acc, u_buf, zero_buf, count,
           l_sem, w_sem, a_sem, out_sem, send_sem):
    row_size, col_size, rep_size = sizes
    rows_blk, cols_blk, blk, _ = a_ref.shape
    num = rows_blk * row_size
    chips = col_size * rep_size
    ring = chips * row_size
    slots = a_row.shape[0]
    twin = max(num - ring, 0)
    row, col, rep = lax.axis_index("row"), lax.axis_index("col"), lax.axis_index("rep")

    def snake(y, x):
        return jnp.where(rem(y, 2) == 0, x, col_size - 1 - x)

    chip = rep * col_size + snake(rep, col)
    me = chip * row_size + row

    def place(other_chip, other_row):
        y = div(other_chip, col_size)
        return {"rep": y, "col": snake(y, other_chip - y * col_size), "row": other_row}

    def last_row(dev):
        return jnp.where(dev >= ring - twin, dev + twin, dev)

    def chip_at(y, x):
        return y * col_size + snake(y, x)

    def chip_last(other_chip):
        return last_row(other_chip * row_size + row_size - 1)

    def owner_of(big):
        return jnp.where(big >= ring, big - twin, big)

    my_last = last_row(me)

    def goes_x_first(y):
        return (row == 0) | (y == rep_size - 2)

    x_first = goes_x_first(rep)

    def packed(big, small):
        return div(big * (big + 1), 2) + small

    def send(src, dst, sem, where):
        count[0] = count[0] + 1
        pltpu.make_async_remote_copy(
            src_ref=src, dst_ref=dst, send_sem=send_sem, recv_sem=sem,
            device_id=where, device_id_type=MESH,
        ).start()

    def wait_block(ref, sem):
        pltpu.make_async_copy(ref, ref, sem).wait()

    barrier = pltpu.get_barrier_semaphore()

    @pl.loop(1, ring)
    def _(t):
        dev = rem(me + t, ring)
        pl.semaphore_signal(
            barrier, inc=1, device_id=place(div(dev, row_size), rem(dev, row_size)), device_id_type=MESH)

    count[0] = 0
    zero_buf[...] = jnp.zeros_like(zero_buf)
    d_acc[...] = jnp.zeros_like(d_acc)

    pl.semaphore_wait(barrier, ring - 1)

    def clear_above():
        @pl.loop(0, rows_blk)
        def _(i):
            first = div(i * row_size + row - col + col_size, col_size)

            @pl.loop(jnp.maximum(first, 0), cols_blk)
            def _(j):
                pltpu.make_async_copy(zero_buf, out_ref.at[i, j], out_sem).start()

    def deal(jj):
        j = jj * col_size + col
        for to_col in range(col_size):
            for s in range(slots):
                dev = chip_at(rep, to_col) * row_size + row
                big = dev + s * twin
                real = j <= big
                if s:
                    real = real & (dev >= ring - twin)

                @pl.when(real)
                def _():
                    src, dst = a_ref.at[div(big, row_size), jj], a_row.at[s, j]

                    @pl.when(col == to_col)
                    def _():
                        pltpu.make_async_copy(src, dst, a_sem.at[s, j]).start()

                    @pl.when(col != to_col)
                    def _():
                        send(src, dst, a_sem.at[s, j], {"col": to_col})

    def to_partner(ref, sem, big):
        for other in range(row_size):
            @pl.when((row != other) & (last_row(chip * row_size + other) > big))
            def _():
                send(ref, ref, sem, {"row": other})

    def to_chips(ref, sem, big, lo, hi, both):
        @pl.loop(lo, hi)
        def _(t):
            dest = rem(chip + t, chips)
            for shift in range(row_size):
                core = rem(row + row_size - 1 - shift, row_size)
                wanted = last_row(dest * row_size + core) > big
                if shift < row_size - 1:
                    wanted = wanted & (t <= both)

                @pl.when(wanted)
                def _():
                    send(ref, ref, sem, place(dest, core))

    def to_col_peers(ref, sem, big, whole):
        for shift in range(1, col_size):
            x = rem(col + shift, col_size)
            wanted = chip_last(chip_at(jnp.where(whole, rep_size - 1, rep), x)) > big

            @pl.when(wanted)
            def _():
                send(ref, ref, sem, {"col": x})

    def to_rep_peers(ref, sem, big, whole):
        for shift in range(1, rep_size):
            y = rem(rep + shift, rep_size)
            wanted = jnp.where(whole, chip_last(y * col_size + col_size - 1), chip_last(chip_at(y, col))) > big

            @pl.when(wanted)
            def _():
                send(ref, ref, sem, {"rep": y})

    def arrived(idx, big, small):
        to_partner(l_st.at[idx], l_sem.at[idx], big)

        @pl.when(my_last > big)
        def _():
            held_output(idx, big, small)

    def passed_down(small):
        return small < num - 1 - LAG - rep_size

    def reaches(big, small, x):
        there = chip_at(rep, x)
        relays = x_first & (big - small > NEAR) & (chip_last(chip_at(rep_size - 1, x)) > big)
        return (last_row(there * row_size + row) > big) | relays

    def own_output(idx, big, small, diagonal):
        src, dst = l_st.at[idx], out_ref.at[div(big, row_size), div(small, col_size)]
        to_col = rem(small, col_size)
        down = passed_down(small) & (big != small)

        @pl.when(to_col == col)
        def _():
            pltpu.make_async_copy(src, dst, out_sem).start()

        @pl.when(down & (to_col != col) & jnp.logical_not(reaches(big, small, to_col)))
        def _():
            send(src, src, l_sem.at[idx], {"col": to_col})

        @pl.when(jnp.logical_not(down))
        def _():
            for to_rep in range(rep_size):
                dest = chip_at(jnp.int32(to_rep), to_col) * row_size + row

                @pl.when((dest != me) & (diagonal | (last_row(dest) <= big)))
                def _():
                    send(src, dst, out_sem, {"rep": to_rep, "col": to_col})

    def held_output(idx, big, small):
        @pl.when((rem(big, row_size) == row) & (rem(small, col_size) == col))
        def _():
            pltpu.make_async_copy(
                l_st.at[idx], out_ref.at[div(big, row_size), div(small, col_size)], out_sem).start()

    deal(0)
    deal(1)

    @pl.when(me >= ring // 2)
    def _():
        clear_above()


    @pl.loop(-1, num - 1)
    def _(i):
        @pl.when((i >= 0) & (rem(i, col_size) == 0) & (div(i, col_size) + 2 < cols_blk))
        def _():
            deal(div(i, col_size) + 2)

        owner = owner_of(i)
        owner_chip = div(owner, row_size)
        before = owner_chip == rem(chip + chips - 1, chips)
        same_core = rem(i, row_size) == row
        waits = (i >= 0) & (my_last > i) & (owner != me)

        far = jnp.maximum(i - NEAR, 0)
        theirs = packed(i, 0)

        @pl.when(waits & jnp.logical_not(same_core & (owner_chip != chip)))
        def _():
            @pl.loop(0, far)
            def _(j):
                wait_block(l_st.at[theirs + j], l_sem.at[theirs + j])

        def wait_near():
            @pl.loop(far, i)
            def _(j):
                idx = theirs + j
                wait_block(l_st.at[idx], l_sem.at[idx])

                @pl.when(same_core & (owner_chip != chip))
                def _():
                    @pl.when(jnp.logical_not(before))
                    def _():
                        to_partner(l_st.at[idx], l_sem.at[idx], i)

                    held_output(idx, i, j)

        @pl.loop(0, slots)
        def _(s):
            big = me + s * twin
            idx = packed(big, i)
            real = (s == 0) | (me >= ring - twin)
            critical = real & (big == i + 1)
            follow = real & (big > i) & (i >= 0)

            @pl.when(follow)
            def _():
                mine = packed(big, 0)
                first_slot = (s == 0) | (me <= i)
                acc[...] = jnp.zeros_like(acc)
                quads = div(far, UNROLL)

                @pl.loop(0, quads)
                def _(g):
                    base = g * UNROLL
                    acc[...] += dot_nt(
                        jnp.concatenate([l_st[mine + base + u] for u in range(UNROLL)], axis=1),
                        jnp.concatenate([l_st[theirs + base + u] for u in range(UNROLL)], axis=1))

                @pl.when(waits & first_slot)
                def _():
                    wait_near()

                @pl.loop(quads, div(i + UNROLL - 1, UNROLL))
                def _(g):
                    base = g * UNROLL
                    last = [jnp.minimum(base + u, i - 1) for u in range(UNROLL)]
                    acc[...] += dot_nt(
                        jnp.concatenate([jnp.where(base + u < i, l_st[mine + last[u]], 0.0) for u in range(UNROLL)], axis=1),
                        jnp.concatenate([l_st[theirs + last[u]] for u in range(UNROLL)], axis=1))

                wait_block(a_row.at[s, i], a_sem.at[s, i])
                rest = a_row[s, i] - acc[...]

                @pl.when(waits & first_slot)
                def _():
                    wait_block(w_st.at[i], w_sem.at[i])

                    @pl.when(same_core & (owner_chip != chip) & jnp.logical_not(before))
                    def _():
                        to_partner(w_st.at[i], w_sem.at[i], i)

                l_new = dot_nt(rest, w_st[i])
                l_st[idx] = l_new
                new, new_sem = l_st.at[idx], l_sem.at[idx]
                near = big - i <= NEAR
                to_partner(new, new_sem, big)

                @pl.when(near)
                def _():
                    to_chips(new, new_sem, big, 1, jnp.where(critical, 2, chips), 1)

                @pl.when(jnp.logical_not(near))
                def _():
                    to_col_peers(new, new_sem, big, x_first)
                    to_rep_peers(new, new_sem, big, jnp.logical_not(x_first))

                @pl.when(jnp.logical_not(critical))
                def _():
                    own_output(idx, big, i, False)

                d_acc[s] = d_acc[s] + dot_nt(l_new, l_new)

            @pl.when(critical)
            def _():
                wait_block(a_row.at[s, big], a_sem.at[s, big])
                acc[...] = a_row[s, big] - d_acc[s]

                def put_u(p, val):
                    u_buf[SUB * p:SUB * p + SUB, :] = val

                def put_w(p, val):
                    w_st[big, SUB * p:SUB * p + SUB, :] = val

                factor_block([acc[SUB * q:SUB * q + SUB, :] for q in range(blk // SUB)], put_u, put_w)
                to_partner(w_st.at[big], w_sem.at[big], big)
                to_chips(w_st.at[big], w_sem.at[big], big, 1, chips, 1)

                @pl.when(follow)
                def _():
                    to_chips(l_st.at[idx], l_sem.at[idx], big, 2, chips, 1)
                    own_output(idx, big, i, False)

                lane = lax.broadcasted_iota(jnp.int32, (blk, blk), 1)
                sub = lax.broadcasted_iota(jnp.int32, (blk, blk), 0)
                diag = packed(big, big)
                l_st[diag] = jnp.where(lane <= sub, u_buf[...].T, 0.0)
                own_output(diag, big, big, True)

                @pl.when((s == 0) & (me < ring // 2))
                def _():
                    clear_above()

        soon = (me == i + 2) | ((me >= ring - twin) & (me + twin == i + 2))
        now = (me == i + 1) | ((me >= ring - twin) & (me + twin == i + 1))

        @pl.loop(jnp.where(now, jnp.maximum(i - 1, -1), i), jnp.where(soon, i, i + 1))
        def _(q):
            def relay(source, along):
                for s in range(slots):
                    big = source + s * twin
                    real = big - q >= NEAR
                    if s:
                        real = real & (source >= ring - twin)
                    if along == "rep":
                        real = real & (chip_last(chip_at(rep_size - 1, col)) > big)
                    else:
                        real = real & (chip_last(rep * col_size + col_size - 1) > big)

                    @pl.when(real)
                    def _():
                        idx = packed(big, q - 1)
                        wait_block(l_st.at[idx], l_sem.at[idx])
                        if along == "rep":
                            to_rep_peers(l_st.at[idx], l_sem.at[idx], big, False)
                        else:
                            to_col_peers(l_st.at[idx], l_sem.at[idx], big, False)
                        arrived(idx, big, q - 1)

            @pl.when((q >= 1) & x_first)
            def _():
                for shift in range(1, col_size):
                    relay(chip_at(rep, rem(col + shift, col_size)) * row_size + row, "rep")

            for shift in range(1, rep_size):
                other = rem(rep + shift, rep_size)

                @pl.when((q >= 1) & jnp.logical_not(goes_x_first(other)))
                def _():
                    relay(chip_at(other, col) * row_size + row, "col")

            @pl.when(q >= NEAR)
            def _():
                first = q + 1 + rem(q + 1 + row, row_size)

                @pl.loop(0, div(jnp.maximum(my_last - first, 0) + row_size - 1, row_size))
                def _(t):
                    j = first + t * row_size
                    source = div(owner_of(j), row_size)
                    y = div(source, col_size)
                    second = jnp.where(goes_x_first(y), y != rep, snake(y, source - y * col_size) != col)

                    @pl.when(second)
                    def _():
                        idx = packed(j, q - NEAR)
                        wait_block(l_st.at[idx], l_sem.at[idx])
                        arrived(idx, j, q - NEAR)

            @pl.loop(0, rep_size)
            def _(gap):
                small = q - LAG - gap
                y = rep + gap

                @pl.when((small >= 0) & (rem(jnp.maximum(small, 0), col_size) == col) & (y < rep_size) & passed_down(small))
                def _():
                    @pl.loop(0, col_size)
                    def _(x):
                        dev = chip_at(y, x) * row_size + row

                        for s in range(slots):
                            big = dev + s * twin
                            real = big > small
                            if s:
                                real = real & (dev >= ring - twin)

                            @pl.when(real)
                            def _():
                                idx = packed(big, small)
                                held = (gap == 0) & ((dev == me) | (my_last > big))

                                @pl.when(jnp.where(gap == 0, (dev != me) & jnp.logical_not(reaches(big, small, col)), True))
                                def _():
                                    wait_block(l_st.at[idx], l_sem.at[idx])

                                @pl.when(jnp.logical_not(held))
                                def _():
                                    held_output(idx, big, small)

                                @pl.when(rep > 0)
                                def _():
                                    send(l_st.at[idx], l_st.at[idx], l_sem.at[idx], {"rep": rep - 1})

    chunk = 16

    @pl.loop(0, div(count[0], chunk))
    def _(t):
        wait_block(l_st.at[0:chunk], send_sem)

    @pl.loop(0, rem(count[0], chunk))
    def _(t):
        wait_block(l_st.at[0], send_sem)

    wait_block(out_ref, out_sem)


def solution(mesh):
    sizes = tuple(mesh.shape[axis] for axis in ("row", "col", "rep"))
    grid_spec = P(("b", "row"), "col")

    def local_factor(a_loc):
        rows_blk, cols_blk, blk, _ = a_loc.shape
        num = rows_blk * sizes[0]
        ring = sizes[0] * sizes[1] * sizes[2]
        slots = -(-num // ring)
        assert slots <= 2
        f32 = jnp.float32
        dma = pltpu.SemaphoreType.DMA
        tri = num * (num + 1) // 2
        return pl.pallas_call(
            functools.partial(kernel, sizes),
            out_shape=jax.ShapeDtypeStruct(a_loc.shape, f32),
            in_specs=[pl.BlockSpec(memory_space=pl.ANY)],
            out_specs=pl.BlockSpec(memory_space=pl.ANY),
            scratch_shapes=[
                pltpu.VMEM((tri, blk, blk), f32),
                pltpu.VMEM((num, blk, blk), f32),
                pltpu.VMEM((slots, num, blk, blk), f32),
                pltpu.VMEM((slots, blk, blk), f32),
                pltpu.VMEM((blk, blk), f32),
                pltpu.VMEM((blk, blk), f32),
                pltpu.VMEM((blk, blk), f32),
                pltpu.SMEM((1,), jnp.int32),
                dma((tri,)),
                dma((num,)),
                dma((slots, num)),
                dma,
                dma,
            ],
            compiler_params=pltpu.CompilerParams(
                collective_id=0, has_side_effects=True, vmem_limit_bytes=67043328,
            ),
        )(a_loc)

    return jax.shard_map(local_factor, mesh=mesh, in_specs=grid_spec, out_specs=grid_spec, check_vma=False)
```
